128 devices in a mesh: row: 32 (over z, y, core), col: 4 (over x).
Axes of the slice: x: 4, y: 4, z: 4, core: 2. Of those that a mesh axis runs over, the one named last changes fastest.
Arguments:
- tracer: float32 [512, 512, 512], P(None, 'row', 'col'), may hold values from -6 to 6
- symbol_x: float32 [512], replicated, may hold values from 0.3 to 3
- symbol_y: float32 [512], replicated, may hold values from 0.3 to 3
- symbol_z: float32 [512], replicated, may hold values from 0.3 to 3
Outputs:
- spectrum: float32 [512, 512, 512], P('row', 'col')
The draws below stay inside these ranges and needn't reach their ends.
All inputs are finite; a program needn't handle non-finite values.
Results may differ from the reference program's by a relative error of at most 0.000075.
Values sent between devices are 32-bit elements; how exact they have to be, the bound alone decides.
A program may use at most 64 MiB of HBM per device.

```python
import jax
import jax.numpy as jnp
from jax import lax

GRID_X = 512
GRID_Y = 512
GRID_Z = 512


def level_of(stream_key, extent, shards, smallest, largest):
    def one(axis_at, shards_of):
        draws = jax.random.uniform(jax.random.fold_in(jax.random.fold_in(stream_key, 6), axis_at), (shards_of,), jnp.float32, smallest / len(shards), largest / len(shards))
        return jnp.repeat(jnp.exp(draws), extent[axis_at] // shards_of).reshape((-1,) + (1,) * (len(extent) - axis_at - 1))

    level = one(*shards[0])
    for cut in shards[1:]:
        level = level * one(*cut)
    return level


def gaussian(key, dims, deviation, most, cuts=(), dtype=jnp.bfloat16):
    loudness = level_of(key, dims, cuts, -0.22, 0.18) if cuts else 1.0
    values = jax.random.normal(key, dims, jnp.float32) * deviation * loudness
    return jnp.minimum(jnp.maximum(values, -most), most).astype(dtype)


def setup_inputs(seed: int = 0) -> dict:
    seeds = jax.random.split(jax.random.key(seed), 5)
    return {
        "tracer": gaussian(seeds[0], (GRID_X, GRID_Y, GRID_Z), 1.0, 6.0, ((1, 32), (2, 4)), jnp.float32),
        "symbol_x": jnp.clip(jax.random.uniform(seeds[1], (GRID_X,), jnp.float32, 0.3, 3.0), 0.3, 3.0),
        "symbol_y": jnp.clip(jax.random.uniform(seeds[2], (GRID_Y,), jnp.float32, 0.3, 3.0), 0.3, 3.0),
        "symbol_z": jnp.clip(jax.random.uniform(seeds[3], (GRID_Z,), jnp.float32, 0.3, 3.0), 0.3, 3.0),
    }


def transform_table(count):
    rank = jnp.arange(count)
    angle = (jnp.pi / (count + 1)) * (((rank[:, None] + 1) * (rank[None, :] + 1)) % (2 * count + 2)).astype(jnp.float32)
    return jnp.sin(angle) * (2.0 / (count + 1)) ** 0.5


def to_modes(values, dim):
    moved = jnp.tensordot(values, transform_table(values.shape[dim]), axes=([dim], [0]), precision=lax.Precision.HIGHEST)
    return jnp.moveaxis(moved, -1, dim)


def reference(tracer, symbol_x, symbol_y, symbol_z):
    spectrum = tracer
    spectrum = to_modes(spectrum, 0)
    spectrum = to_modes(spectrum, 1)
    spectrum = to_modes(spectrum, 2)
    symbol = symbol_x[:, None, None] + symbol_y[None, :, None] + symbol_z[None, None, :]
    spectrum = spectrum * ((1.0 - 0.2 * symbol) / (1.0 + 0.2 * symbol))
    return spectrum
```

```python
import functools

import jax
import jax.numpy as jnp
import numpy as np
from jax import lax
from jax.experimental import pallas as pl
from jax.experimental.pallas import tpu as pltpu
from jax.sharding import PartitionSpec as P

MESH = pl.DeviceIdType.MESH
PER_CHUNK = 1
AHEAD = 2


def transform_table(count):
    rank = np.arange(1, count + 1, dtype=np.int64)
    angle = (np.pi / (count + 1)) * ((rank[:, None] * rank[None, :]) % (2 * count + 2))
    return np.sin(angle) * np.sqrt(2.0 / (count + 1))


def halves(table):
    high = table.astype(jnp.bfloat16)
    low = (table - high.astype(np.float64)).astype(jnp.bfloat16)
    return high, low


def split(values):
    high = values.astype(jnp.bfloat16)
    return high, (values - high.astype(jnp.float32)).astype(jnp.bfloat16)


def dot(a, b):
    return jnp.dot(a, b, preferred_element_type=jnp.float32)


def kernel(
    rows,
    cols,
    field_hbm,
    table_x_hbm,
    table_hbm,
    symbol_x,
    symbol_y,
    symbol_z,
    out,
    field,
    high,
    low,
    table_x,
    table,
    outgoing,
    lines_y,
    turned,
    lines_z,
    field_sem,
    table_sem,
    row_send,
    row_recv,
    col_send,
    col_recv,
):
    row, col = lax.axis_index("row"), lax.axis_index("col")
    planes = field.shape[0]
    chunks, _, sent, wide = outgoing.shape
    per = sent // rows
    size_y = lines_y.shape[1]
    part_y = lines_z.shape[2]
    size = field.shape[1]

    barrier = pltpu.get_barrier_semaphore()

    def greet_row(step, _):
        pl.semaphore_signal(
            barrier, inc=1, device_id=(lax.rem(row + step, rows), col), device_id_type=MESH
        )
        return 0

    lax.fori_loop(1, rows, greet_row, 0)
    for step in range(1, cols):
        pl.semaphore_signal(
            barrier, inc=1, device_id=(row, lax.rem(col + step, cols)), device_id_type=MESH
        )

    load_x = pltpu.make_async_copy(table_x_hbm, table_x, table_sem.at[0])
    load_x.start()
    loads = [
        pltpu.make_async_copy(field_hbm.at[:, plane, :], field.at[plane], field_sem.at[plane])
        for plane in range(planes)
    ]
    for load in loads:
        load.start()
    load_table = pltpu.make_async_copy(table_hbm, table, table_sem.at[1])
    load_table.start()

    def along_x(chunk, pair):
        mine = table_x.at[chunk]
        both = dot(mine[...], high[pair])
        got = both[:sent] + both[sent:] + dot(mine[pl.ds(0, sent), :], low[pair])
        outgoing[chunk, 2 * pair] = got[:, :wide]
        outgoing[chunk, 2 * pair + 1] = got[:, wide:]

    def send_row(chunk):
        def to_peer(step, _):
            peer = lax.rem(row + step, rows)
            for mode in range(per):
                pltpu.make_async_remote_copy(
                    src_ref=outgoing.at[chunk, :, peer * per + mode, :],
                    dst_ref=lines_y.at[
                        chunk * per + mode, pl.ds(pl.multiple_of(row * planes, planes), planes), :
                    ],
                    send_sem=row_send,
                    recv_sem=row_recv.at[chunk],
                    device_id=(peer, col),
                    device_id_type=MESH,
                ).start()
            return 0

        lax.fori_loop(1, rows, to_peer, 0)
        for mode in range(per):
            for plane in range(planes):
                lines_y[chunk * per + mode, pl.ds(row * planes + plane, 1), :] = outgoing[
                    chunk, plane, pl.ds(row * per + mode, 1), :
                ]

    load_x.wait()
    for pair in range(planes // 2):
        loads[2 * pair].wait()
        loads[2 * pair + 1].wait()
        both = jnp.concatenate([field[2 * pair], field[2 * pair + 1]], axis=1)
        high[pair], low[pair] = split(both)
        along_x(0, pair)
    pl.semaphore_wait(barrier, rows - 1 + cols - 1)
    send_row(0)

    def next_chunk(chunk):
        for pair in range(planes // 2):
            along_x(chunk, pair)
        send_row(chunk)

    for chunk in range(1, AHEAD):
        next_chunk(chunk)
    load_table.wait()

    def along_y(chunk):
        arrived = lines_y.at[pl.ds(chunk * per, per), pl.ds(0, size_y - planes), :]
        pltpu.make_async_remote_copy(
            arrived, arrived, row_send, row_recv.at[chunk], device_id=(row, col), device_id_type=MESH
        ).wait_recv()
        for mode in range(per):
            above, below = split(lines_y[chunk * per + mode])
            got = dot(table[0], above) + dot(table[1], above) + dot(table[0], below)
            turned[chunk * per + mode] = got
        for step in range(1, cols):
            peer = lax.rem(col + step, cols)
            pltpu.make_async_remote_copy(
                src_ref=turned.at[
                    pl.ds(chunk * per, per), pl.ds(pl.multiple_of(peer * part_y, part_y), part_y), :
                ],
                dst_ref=lines_z.at[col, pl.ds(chunk * per, per)],
                send_sem=col_send,
                recv_sem=col_recv.at[chunk],
                device_id=(row, peer),
                device_id_type=MESH,
            ).start()
        for mode in range(per):
            lines_z[col, chunk * per + mode] = turned[
                chunk * per + mode, pl.ds(pl.multiple_of(col * part_y, part_y), part_y), :
            ]

    def along_z(chunk):
        arrived = lines_z.at[pl.ds(0, cols - 1), pl.ds(chunk * per, per)]
        pltpu.make_async_remote_copy(
            arrived, arrived, col_send, col_recv.at[chunk], device_id=(row, col), device_id_type=MESH
        ).wait_recv()
        for mode in range(per):
            at = chunk * per + mode
            line = jnp.concatenate([lines_z[part, at] for part in range(cols)], axis=1)
            above, below = split(line)
            got = dot(above, table[0]) + dot(above, table[1]) + dot(below, table[0])
            symbol = symbol_x[at] + symbol_y[...] + symbol_z[...]
            out[at] = got * (2.0 / (1.0 + 0.2 * symbol) - 1.0)

    def step(chunk, _):
        @pl.when(chunk + AHEAD < chunks)
        def _():
            next_chunk(chunk + AHEAD)

        along_y(chunk)

        @pl.when(chunk >= 1)
        def _():
            along_z(chunk - 1)

        return 0

    lax.fori_loop(0, chunks, step, 0)
    along_z(chunks - 1)
    all_rows = lines_y.at[:, pl.ds(0, size_y - planes), :]
    pltpu.make_async_remote_copy(
        all_rows, all_rows, row_send, row_recv.at[0], device_id=(row, col), device_id_type=MESH
    ).wait_send()
    all_cols = lines_z.at[pl.ds(0, cols - 1)]
    pltpu.make_async_remote_copy(
        all_cols, all_cols, col_send, col_recv.at[0], device_id=(row, col), device_id_type=MESH
    ).wait_send()


def per_device(rows, cols, field, symbol_x, symbol_y, symbol_z):
    size, planes, wide = field.shape
    size_y, size_z = planes * rows, wide * cols
    share, part_y = size // rows, size_y // cols
    per = PER_CHUNK
    chunks = share // per
    sent = rows * per

    high, low = halves(transform_table(size))
    order = np.arange(size).reshape(rows, chunks, per).transpose(1, 0, 2).reshape(chunks, sent)
    table_x = np.concatenate([high[order], low[order]], axis=1)
    table = np.stack([high, low])

    mine_x = lax.dynamic_slice_in_dim(symbol_x, lax.axis_index("row") * share, share)
    mine_y = lax.dynamic_slice_in_dim(symbol_y, lax.axis_index("col") * part_y, part_y)

    vmem = pl.BlockSpec(memory_space=pltpu.VMEM)
    anywhere = pl.BlockSpec(memory_space=pl.ANY)
    return pl.pallas_call(
        functools.partial(kernel, rows, cols),
        out_shape=jax.ShapeDtypeStruct((share, part_y, size_z), jnp.float32),
        in_specs=[anywhere, anywhere, anywhere, pl.BlockSpec(memory_space=pltpu.SMEM), vmem, vmem],
        out_specs=vmem,
        scratch_shapes=[
            pltpu.VMEM((planes, size, wide), jnp.float32),
            pltpu.VMEM((planes // 2, size, 2 * wide), jnp.bfloat16),
            pltpu.VMEM((planes // 2, size, 2 * wide), jnp.bfloat16),
            pltpu.VMEM(table_x.shape, jnp.bfloat16),
            pltpu.VMEM(table.shape, jnp.bfloat16),
            pltpu.VMEM((chunks, planes, sent, wide), jnp.float32),
            pltpu.VMEM((share, size_y, wide), jnp.float32),
            pltpu.VMEM((share, size_y, wide), jnp.float32),
            pltpu.VMEM((cols, share, part_y, wide), jnp.float32),
            pltpu.SemaphoreType.DMA((planes,)),
            pltpu.SemaphoreType.DMA((2,)),
            pltpu.SemaphoreType.DMA,
            pltpu.SemaphoreType.DMA((chunks,)),
            pltpu.SemaphoreType.DMA,
            pltpu.SemaphoreType.DMA((chunks,)),
        ],
        compiler_params=pltpu.CompilerParams(
            collective_id=0, has_side_effects=True, vmem_limit_bytes=60 << 20
        ),
        name="modes",
    )(
        field,
        jnp.asarray(table_x),
        jnp.asarray(table),
        mine_x,
        mine_y[:, None],
        symbol_z[None, :],
    )


def solution(mesh):
    rows, cols = mesh.shape["row"], mesh.shape["col"]
    return jax.shard_map(
        functools.partial(per_device, rows, cols),
        mesh=mesh,
        in_specs=(P(None, "row", "col"), P(), P(), P()),
        out_specs=P("row", "col", None),
        check_vma=False,
    )
```

```python
import functools

import jax
import jax.numpy as jnp
import numpy as np
from jax import lax
from jax.experimental import pallas as pl
from jax.experimental.pallas import tpu as pltpu
from jax.sharding import PartitionSpec as P

MESH = pl.DeviceIdType.MESH
GROUPS = 2
VMEM_LIMIT = 40 << 20


def transform_table(count):
    rank = np.arange(1, count + 1, dtype=np.int64)
    angle = (np.pi / (count + 1)) * ((rank[:, None] * rank[None, :]) % (2 * count + 2))
    return np.sin(angle) * np.sqrt(2.0 / (count + 1))


def halves(table):
    high = table.astype(jnp.bfloat16)
    low = (table - high.astype(np.float64)).astype(jnp.bfloat16)
    return high, low


def modes_of(share, groups):
    half = share // groups // 2
    order = []
    for group in range(groups):
        first = list(range(group * half, (group + 1) * half))
        order.append(first + [share - 1 - mode for mode in reversed(first)])
    return order


def split(values):
    high = values.astype(jnp.bfloat16)
    return high, (values - high.astype(jnp.float32)).astype(jnp.bfloat16)


def dot(a, b):
    return jnp.dot(a, b, preferred_element_type=jnp.float32)


def kernel(
    rows,
    cols,
    field_hbm,
    table_x_hbm,
    table_y_hbm,
    table_z_hbm,
    symbol_x_hbm,
    symbol_y_hbm,
    symbol_z_hbm,
    out,
    field,
    high,
    low,
    table_x,
    table_y,
    table_z,
    symbol_x,
    symbol_y,
    symbol_z,
    symbol_yz,
    outgoing,
    lines_y,
    turned,
    lines_z,
    field_sem,
    table_sem,
    row_send,
    row_recv,
    col_send,
    col_recv,
):
    row, col = lax.axis_index("row"), lax.axis_index("col")
    share, part_y, _ = out.shape
    planes, _, half, wide = field.shape
    groups, _, _, lots, _ = outgoing.shape
    size = 2 * half
    in_group = share // groups
    middle = rows // 2
    upper = row // middle
    place = pl.multiple_of((row + upper * (rows + middle - 1 - 2 * row)) * planes, planes)

    barrier = pltpu.get_barrier_semaphore()

    def greet_row(step, _):
        pl.semaphore_signal(
            barrier, inc=1, device_id=(lax.rem(row + step, rows), col), device_id_type=MESH
        )
        return 0

    loads = []
    load_x = pltpu.make_async_copy(table_x_hbm, table_x, table_sem.at[0])
    load_x.start()
    for plane in range(planes):
        source = plane + upper * (planes - 1 - 2 * plane)
        for parity in range(2):
            loads.append(
                pltpu.make_async_copy(
                    field_hbm.at[:, parity, source, :],
                    field.at[plane, parity],
                    field_sem.at[2 * plane + parity],
                )
            )
            loads[-1].start()
    later = [
        pltpu.make_async_copy(source, target, table_sem.at[1 + at])
        for at, (source, target) in enumerate(
            [
                (table_y_hbm, table_y),
                (table_z_hbm, table_z),
                (symbol_x_hbm, symbol_x),
                (symbol_y_hbm, symbol_y),
                (symbol_z_hbm, symbol_z),
            ]
        )
    ]
    for load in later:
        load.start()
    lax.fori_loop(1, rows, greet_row, 0)
    for step in range(1, cols):
        pl.semaphore_signal(
            barrier, inc=1, device_id=(row, lax.rem(col + step, cols)), device_id_type=MESH
        )

    def along_x(group, pair):
        parts = []
        for parity in range(2):
            mine = table_x.at[group, parity]
            both = dot(mine[...], high[pair, parity])
            parts.append(
                both[:lots] + both[lots:] + dot(mine[pl.ds(0, lots), :], low[pair, parity])
            )
        for sign, got in enumerate((parts[0] + parts[1], parts[0] - parts[1])):
            outgoing[group, sign, 2 * pair] = got[:, :wide]
            outgoing[group, sign, 2 * pair + 1] = got[:, wide:]

    def lot_of(chunk, peer):
        group, at = chunk // in_group, lax.rem(chunk, in_group)
        sign = peer // middle
        lot = (at + sign * (in_group - 1 - 2 * at)) * middle + peer + sign * (rows - 1 - 2 * peer)
        return group, sign, lot

    def send_row(chunk):
        def to_peer(step, _):
            peer = lax.rem(row + step, rows)
            group, sign, lot = lot_of(chunk, peer)
            pltpu.make_async_remote_copy(
                src_ref=outgoing.at[group, sign, :, lot, :],
                dst_ref=lines_y.at[chunk, pl.ds(place, planes), :],
                send_sem=row_send,
                recv_sem=row_recv.at[chunk],
                device_id=(peer, col),
                device_id_type=MESH,
            ).start()
            return 0

        lax.fori_loop(1, rows, to_peer, 0)
        group, sign, lot = lot_of(chunk, row)
        for plane in range(planes):
            lines_y[chunk, pl.ds(place + plane, 1), :] = outgoing[
                group, sign, plane, pl.ds(lot, 1), :
            ]

    load_x.wait()
    for pair in range(planes // 2):
        for parity in range(2):
            loads[4 * pair + parity].wait()
            loads[4 * pair + 2 + parity].wait()
            both = jnp.concatenate([field[2 * pair, parity], field[2 * pair + 1, parity]], axis=1)
            high[pair, parity], low[pair, parity] = split(both)
        along_x(0, pair)
    pl.semaphore_wait(barrier, rows - 1 + cols - 1)
    for chunk in range(in_group):
        send_row(chunk)

    for load in later:
        load.wait()
    mine_y = jnp.broadcast_to(
        symbol_y[:, pl.ds(pl.multiple_of(col * part_y, part_y), part_y)], (part_y, part_y)
    )
    symbol_yz[...] = jnp.transpose(mine_y)[:, :1] + symbol_z[...]

    def along_y(chunk):
        arrived = lines_y.at[chunk, pl.ds(0, size - planes), :]
        pltpu.make_async_remote_copy(
            arrived, arrived, row_send, row_recv.at[chunk], device_id=(row, col), device_id_type=MESH
        ).wait_recv()
        first, second = lines_y[chunk, pl.ds(0, half), :], lines_y[chunk, pl.ds(half, half), :]
        above, below = split(jnp.concatenate([first + second, first - second], axis=1))
        got = dot(table_y[0], above) + dot(table_y[1], above) + dot(table_y[0], below)
        turned[chunk, pl.ds(0, half, 2), :] = got[:half, :wide]
        turned[chunk, pl.ds(1, half, 2), :] = got[half:, wide:]
        for step in range(1, cols):
            peer = lax.rem(col + step, cols)
            pltpu.make_async_remote_copy(
                src_ref=turned.at[
                    chunk, pl.ds(pl.multiple_of(peer * part_y, part_y), part_y), :
                ],
                dst_ref=lines_z.at[col, chunk],
                send_sem=col_send,
                recv_sem=col_recv.at[chunk],
                device_id=(row, peer),
                device_id_type=MESH,
            ).start()
        lines_z[col, chunk] = turned[
            chunk, pl.ds(pl.multiple_of(col * part_y, part_y), part_y), :
        ]

    def along_z(chunk):
        arrived = lines_z.at[pl.ds(0, cols - 1), chunk]
        pltpu.make_async_remote_copy(
            arrived, arrived, col_send, col_recv.at[chunk], device_id=(row, col), device_id_type=MESH
        ).wait_recv()
        group, at = chunk // in_group, lax.rem(chunk, in_group)
        tail = at // (in_group // 2)
        mode = group * (in_group // 2) + at + tail * (share - in_group - group * in_group)
        above, below = split(jnp.concatenate([lines_z[part, chunk] for part in range(cols)], axis=1))
        got = dot(above, table_z[0]) + dot(above, table_z[1]) + dot(below, table_z[0])
        symbol = symbol_x[row * share + mode] + symbol_yz[...]
        out[mode] = got * (2.0 / (1.0 + 0.2 * symbol) - 1.0)

    def step(chunk, _):
        along_y(chunk)

        for group in range(1, groups):

            @pl.when(chunk == (group - 1) * in_group + 1)
            def _():
                for pair in range(planes // 2):
                    along_x(group, pair)

        @pl.when(jnp.logical_and(chunk >= 1, chunk + in_group - 1 < share))
        def _():
            send_row(chunk + in_group - 1)

        @pl.when(chunk >= 1)
        def _():
            along_z(chunk - 1)

        return 0

    lax.fori_loop(0, share, step, 0)
    along_z(share - 1)
    all_rows = lines_y.at[:, pl.ds(0, size - planes), :]
    pltpu.make_async_remote_copy(
        all_rows, all_rows, row_send, row_recv.at[0], device_id=(row, col), device_id_type=MESH
    ).wait_send()
    all_cols = lines_z.at[pl.ds(0, cols - 1)]
    pltpu.make_async_remote_copy(
        all_cols, all_cols, col_send, col_recv.at[0], device_id=(row, col), device_id_type=MESH
    ).wait_send()


def per_device(rows, cols, field, symbol_x, symbol_y, symbol_z):
    size, planes, wide = field.shape
    share, part_y = size // rows, size // cols
    half, middle = size // 2, rows // 2

    table = transform_table(size)
    high, low = halves(table)
    order = np.asarray(modes_of(share, GROUPS))
    lots = order.shape[1] * middle
    wanted = (order[:, :, None] + share * np.arange(middle)).reshape(GROUPS, lots)
    table_x = np.stack(
        [np.concatenate([part[wanted] for part in (high, low)], axis=1)[:, :, parity::2] for parity in (0, 1)],
        axis=1,
    )
    table_y = np.stack(
        [np.concatenate([part[0::2, :half], part[1::2, :half]]) for part in (high, low)]
    )
    table_z = np.stack([high, low])

    anywhere = pl.BlockSpec(memory_space=pl.ANY)
    return pl.pallas_call(
        functools.partial(kernel, rows, cols),
        out_shape=pltpu.VMEM((share, part_y, size), jnp.float32),
        in_specs=[anywhere] * 7,
        out_specs=pl.BlockSpec(memory_space=pltpu.VMEM),
        scratch_shapes=[
            pltpu.VMEM((planes, 2, half, wide), jnp.float32),
            pltpu.VMEM((planes // 2, 2, half, 2 * wide), jnp.bfloat16),
            pltpu.VMEM((planes // 2, 2, half, 2 * wide), jnp.bfloat16),
            pltpu.VMEM(table_x.shape, jnp.bfloat16),
            pltpu.VMEM(table_y.shape, jnp.bfloat16),
            pltpu.VMEM(table_z.shape, jnp.bfloat16),
            pltpu.SMEM((size,), jnp.float32),
            pltpu.VMEM((1, size), jnp.float32),
            pltpu.VMEM((1, size), jnp.float32),
            pltpu.VMEM((part_y, size), jnp.float32),
            pltpu.VMEM((GROUPS, 2, planes, lots, wide), jnp.float32),
            pltpu.VMEM((share, size, wide), jnp.float32),
            pltpu.VMEM((share, size, wide), jnp.float32),
            pltpu.VMEM((cols, share, part_y, wide), jnp.float32),
            pltpu.SemaphoreType.DMA((2 * planes,)),
            pltpu.SemaphoreType.DMA((6,)),
            pltpu.SemaphoreType.DMA,
            pltpu.SemaphoreType.DMA((share,)),
            pltpu.SemaphoreType.DMA,
            pltpu.SemaphoreType.DMA((share,)),
        ],
        compiler_params=pltpu.CompilerParams(
            collective_id=0, has_side_effects=True, vmem_limit_bytes=VMEM_LIMIT
        ),
        name="modes",
    )(
        *(
            pltpu.with_memory_space_constraint(operand, pltpu.HBM)
            for operand in (
                field.reshape(half, 2, planes, wide),
                jnp.asarray(table_x),
                jnp.asarray(table_y),
                jnp.asarray(table_z),
                symbol_x,
                symbol_y[None, :],
                symbol_z[None, :],
            )
        )
    )


def solution(mesh):
    rows, cols = mesh.shape["row"], mesh.shape["col"]
    return jax.shard_map(
        functools.partial(per_device, rows, cols),
        mesh=mesh,
        in_specs=(P(None, "row", "col"), P(), P(), P()),
        out_specs=P("row", "col", None),
        check_vma=False,
    )
```

```python
import functools
import math

import jax
import jax.numpy as jnp
import numpy as np
from jax import lax
from jax.experimental import pallas as pl
from jax.experimental.pallas import tpu as pltpu
from jax.sharding import PartitionSpec as P

MESH = pl.DeviceIdType.MESH
CORES = (1, 0)
BEHIND = 3
GROUPS = 2
VMEM_LIMIT = 40 << 20


def transform_table(count):
    rank = np.arange(1, count + 1, dtype=np.int64)
    angle = (np.pi / (count + 1)) * ((rank[:, None] * rank[None, :]) % (2 * count + 2))
    return np.sin(angle) * np.sqrt(2.0 / (count + 1))


def halves(table):
    high = table.astype(jnp.bfloat16)
    low = (table - high.astype(np.float64)).astype(jnp.bfloat16)
    return high, low


def modes_of(share, groups):
    half = share // groups // 2
    order = []
    for group in range(groups):
        first = list(range(group * half, (group + 1) * half))
        order.append(first + [share - 1 - mode for mode in reversed(first)])
    return order


def split(values):
    high = values.astype(jnp.bfloat16)
    return high, (values - high.astype(jnp.float32)).astype(jnp.bfloat16)


def dot(a, b):
    return jnp.dot(a, b, preferred_element_type=jnp.float32)


def kernel(
    rows,
    cols,
    field_hbm,
    table_x_hbm,
    table_y_hbm,
    table_z_hbm,
    symbol_x_hbm,
    symbol_y_hbm,
    symbol_z_hbm,
    out,
    field,
    high,
    low,
    table_x,
    table_y,
    table_z,
    symbol_x,
    symbol_y,
    symbol_z,
    symbol_yz,
    outgoing,
    lines_y,
    turned,
    lines_z,
    field_sem,
    table_sem,
    row_send,
    row_recv,
    col_send,
    col_recv,
):
    row, col = lax.axis_index("row"), lax.axis_index("col")
    share, part_y, _ = out.shape
    planes, _, half, wide = field.shape
    groups, _, _, lots, _ = outgoing.shape
    size = 2 * half
    in_group = share // groups
    middle = rows // 2
    upper = row // middle
    place = pl.multiple_of((row + upper * (rows + middle - 1 - 2 * row)) * planes, planes)

    side = math.isqrt(middle)
    chip, core = row // 2, lax.rem(row, 2)
    peers = []
    for target in CORES:
        for ahead, across in sorted(
            ((a, b) for a in range(side) for b in range(side)),
            key=lambda at: -sum(min(step, side - step) for step in at),
        )[:-1]:
            there = lax.rem(chip // side + ahead, side) * side + lax.rem(chip + across, side)
            peers.append(2 * there + target)
    peers.append(2 * chip + 1 - core)

    barrier = pltpu.get_barrier_semaphore()

    def greet_row(step, _):
        pl.semaphore_signal(
            barrier, inc=1, device_id=(lax.rem(row + step, rows), col), device_id_type=MESH
        )
        return 0

    def load_of(plane, parity, source):
        return pltpu.make_async_copy(
            field_hbm.at[:, parity, source, :],
            field.at[plane, parity],
            field_sem.at[2 * plane + parity],
        )

    load_x = pltpu.make_async_copy(table_x_hbm, table_x, table_sem.at[0])
    load_x.start()

    def load_plane(plane, _):
        source = plane + upper * (planes - 1 - 2 * plane)
        for parity in range(2):
            load_of(plane, parity, source).start()
        return 0

    lax.fori_loop(0, planes, load_plane, 0)
    later = [
        pltpu.make_async_copy(source, target, table_sem.at[1 + at])
        for at, (source, target) in enumerate(
            [
                (table_y_hbm, table_y),
                (table_z_hbm, table_z),
                (symbol_x_hbm, symbol_x),
                (symbol_y_hbm, symbol_y),
                (symbol_z_hbm, symbol_z),
            ]
        )
    ]
    for load in later:
        load.start()
    lax.fori_loop(1, rows, greet_row, 0)
    for step in range(1, cols):
        pl.semaphore_signal(
            barrier, inc=1, device_id=(row, lax.rem(col + step, cols)), device_id_type=MESH
        )

    def along_x(group, pair):
        parts = []
        for parity in range(2):
            mine = table_x.at[group, parity]
            both = dot(mine[...], high[pair, parity])
            parts.append(
                both[:lots] + both[lots:] + dot(mine[pl.ds(0, lots), :], low[pair, parity])
            )
        for sign, got in enumerate((parts[0] + parts[1], parts[0] - parts[1])):
            outgoing[group, sign, 2 * pair] = got[:, :wide]
            outgoing[group, sign, 2 * pair + 1] = got[:, wide:]

    def lot_of(chunk, peer):
        group, at = chunk // in_group, lax.rem(chunk, in_group)
        sign = peer // middle
        lot = (at + sign * (in_group - 1 - 2 * at)) * middle + peer + sign * (rows - 1 - 2 * peer)
        return group, sign, lot

    def send_row(chunk, first=0, count=planes):
        for peer in peers:
            group, sign, lot = lot_of(chunk, peer)
            pltpu.make_async_remote_copy(
                src_ref=outgoing.at[group, sign, pl.ds(first, count), lot, :],
                dst_ref=lines_y.at[chunk, pl.ds(place + first, count), :],
                send_sem=row_send,
                recv_sem=row_recv.at[chunk],
                device_id=(peer, col),
                device_id_type=MESH,
            ).start()

        group, sign, lot = lot_of(chunk, row)
        for plane in range(first, first + count):
            lines_y[chunk, pl.ds(place + plane, 1), :] = outgoing[
                group, sign, plane, pl.ds(lot, 1), :
            ]

    load_x.wait()
    for pair in range(planes // 2):
        for parity in range(2):
            load_of(2 * pair, parity, 2 * pair).wait()
            load_of(2 * pair + 1, parity, 2 * pair + 1).wait()
            both = jnp.concatenate([field[2 * pair, parity], field[2 * pair + 1, parity]], axis=1)
            high[pair, parity], low[pair, parity] = split(both)
        along_x(0, pair)
        if pair == planes // 4 - 1:
            pl.semaphore_wait(barrier, rows - 1 + cols - 1)
            send_row(0, 0, planes // 2)
    send_row(0, planes // 2, planes // 2)

    def send_first(chunk, _):
        send_row(chunk)
        return 0

    lax.fori_loop(1, in_group, send_first, 0)

    for load in later:
        load.wait()
    mine_y = jnp.broadcast_to(
        symbol_y[:, pl.ds(pl.multiple_of(col * part_y, part_y), part_y)], (part_y, part_y)
    )
    symbol_yz[...] = jnp.transpose(mine_y)[:, :1] + symbol_z[...]

    def along_y(chunk):
        arrived = lines_y.at[chunk, pl.ds(0, size - planes), :]
        pltpu.make_async_remote_copy(
            arrived, arrived, row_send, row_recv.at[chunk], device_id=(row, col), device_id_type=MESH
        ).wait_recv()
        first, second = lines_y[chunk, pl.ds(0, half), :], lines_y[chunk, pl.ds(half, half), :]
        above, below = split(jnp.concatenate([first + second, first - second], axis=1))
        got = dot(table_y[0], above) + dot(table_y[1], above) + dot(table_y[0], below)
        turned[chunk, pl.ds(0, half, 2), :] = got[:half, :wide]
        turned[chunk, pl.ds(1, half, 2), :] = got[half:, wide:]
        for step in range(1, cols):
            peer = lax.rem(col + step, cols)
            pltpu.make_async_remote_copy(
                src_ref=turned.at[
                    chunk, pl.ds(pl.multiple_of(peer * part_y, part_y), part_y), :
                ],
                dst_ref=lines_z.at[col, chunk],
                send_sem=col_send,
                recv_sem=col_recv.at[chunk],
                device_id=(row, peer),
                device_id_type=MESH,
            ).start()
        lines_z[col, chunk] = turned[
            chunk, pl.ds(pl.multiple_of(col * part_y, part_y), part_y), :
        ]

    def along_z(chunk):
        arrived = lines_z.at[pl.ds(0, cols - 1), chunk]
        pltpu.make_async_remote_copy(
            arrived, arrived, col_send, col_recv.at[chunk], device_id=(row, col), device_id_type=MESH
        ).wait_recv()
        group, at = chunk // in_group, lax.rem(chunk, in_group)
        tail = at // (in_group // 2)
        mode = group * (in_group // 2) + at + tail * (share - in_group - group * in_group)
        above, below = split(jnp.concatenate([lines_z[part, chunk] for part in range(cols)], axis=1))
        got = dot(above, table_z[0]) + dot(above, table_z[1]) + dot(below, table_z[0])
        symbol = symbol_x[row * share + mode] + symbol_yz[...]
        out[mode] = got * (2.0 / (1.0 + 0.2 * symbol) - 1.0)

    def step(chunk, _):
        along_y(chunk)

        for group in range(1, groups):

            @pl.when(chunk == (group - 1) * in_group + 1)
            def _():
                for pair in range(planes // 2):
                    along_x(group, pair)

        @pl.when(jnp.logical_and(chunk >= 1, chunk + in_group - 1 < share))
        def _():
            send_row(chunk + in_group - 1)

        @pl.when(chunk >= BEHIND)
        def _():
            along_z(chunk - BEHIND)

        return 0

    lax.fori_loop(0, share, step, 0)

    def last(chunk, _):
        along_z(chunk)
        return 0

    lax.fori_loop(share - BEHIND, share, last, 0)
    all_rows = lines_y.at[:, pl.ds(0, size - planes), :]
    pltpu.make_async_remote_copy(
        all_rows, all_rows, row_send, row_recv.at[0], device_id=(row, col), device_id_type=MESH
    ).wait_send()
    all_cols = lines_z.at[pl.ds(0, cols - 1)]
    pltpu.make_async_remote_copy(
        all_cols, all_cols, col_send, col_recv.at[0], device_id=(row, col), device_id_type=MESH
    ).wait_send()


def per_device(rows, cols, field, symbol_x, symbol_y, symbol_z):
    size, planes, wide = field.shape
    share, part_y = size // rows, size // cols
    half, middle = size // 2, rows // 2

    table = transform_table(size)
    high, low = halves(table)
    order = np.asarray(modes_of(share, GROUPS))
    lots = order.shape[1] * middle
    wanted = (order[:, :, None] + share * np.arange(middle)).reshape(GROUPS, lots)
    table_x = np.stack(
        [np.concatenate([part[wanted] for part in (high, low)], axis=1)[:, :, parity::2] for parity in (0, 1)],
        axis=1,
    )
    table_y = np.stack(
        [np.concatenate([part[0::2, :half], part[1::2, :half]]) for part in (high, low)]
    )
    table_z = np.stack([high, low])

    anywhere = pl.BlockSpec(memory_space=pl.ANY)
    return pl.pallas_call(
        functools.partial(kernel, rows, cols),
        out_shape=pltpu.VMEM((share, part_y, size), jnp.float32),
        in_specs=[anywhere] * 7,
        out_specs=pl.BlockSpec(memory_space=pltpu.VMEM),
        scratch_shapes=[
            pltpu.VMEM((planes, 2, half, wide), jnp.float32),
            pltpu.VMEM((planes // 2, 2, half, 2 * wide), jnp.bfloat16),
            pltpu.VMEM((planes // 2, 2, half, 2 * wide), jnp.bfloat16),
            pltpu.VMEM(table_x.shape, jnp.bfloat16),
            pltpu.VMEM(table_y.shape, jnp.bfloat16),
            pltpu.VMEM(table_z.shape, jnp.bfloat16),
            pltpu.SMEM((size,), jnp.float32),
            pltpu.VMEM((1, size), jnp.float32),
            pltpu.VMEM((1, size), jnp.float32),
            pltpu.VMEM((part_y, size), jnp.float32),
            pltpu.VMEM((GROUPS, 2, planes, lots, wide), jnp.float32),
            pltpu.VMEM((share, size, wide), jnp.float32),
            pltpu.VMEM((share, size, wide), jnp.float32),
            pltpu.VMEM((cols, share, part_y, wide), jnp.float32),
            pltpu.SemaphoreType.DMA((2 * planes,)),
            pltpu.SemaphoreType.DMA((6,)),
            pltpu.SemaphoreType.DMA,
            pltpu.SemaphoreType.DMA((share,)),
            pltpu.SemaphoreType.DMA,
            pltpu.SemaphoreType.DMA((share,)),
        ],
        compiler_params=pltpu.CompilerParams(
            collective_id=0, has_side_effects=True, vmem_limit_bytes=VMEM_LIMIT
        ),
        name="modes",
    )(
        *(
            pltpu.with_memory_space_constraint(operand, pltpu.HBM)
            for operand in (
                field.reshape(half, 2, planes, wide),
                jnp.asarray(table_x),
                jnp.asarray(table_y),
                jnp.asarray(table_z),
                symbol_x,
                symbol_y[None, :],
                symbol_z[None, :],
            )
        )
    )


def solution(mesh):
    rows, cols = mesh.shape["row"], mesh.shape["col"]
    return jax.shard_map(
        functools.partial(per_device, rows, cols),
        mesh=mesh,
        in_specs=(P(None, "row", "col"), P(), P(), P()),
        out_specs=P("row", "col", None),
        check_vma=False,
    )
```

```python
import functools
import math

import jax
import jax.numpy as jnp
import numpy as np
from jax import lax
from jax.experimental import pallas as pl
from jax.experimental.pallas import tpu as pltpu
from jax.sharding import PartitionSpec as P

MESH = pl.DeviceIdType.MESH
CORES = (1, 0)
BEHIND = 3
GROUPS = 4
VMEM_LIMIT = 40 << 20


def transform_table(count):
    rank = np.arange(1, count + 1, dtype=np.int64)
    angle = (np.pi / (count + 1)) * ((rank[:, None] * rank[None, :]) % (2 * count + 2))
    return np.sin(angle) * np.sqrt(2.0 / (count + 1))


def halves(table):
    high = table.astype(jnp.bfloat16)
    low = (table - high.astype(np.float64)).astype(jnp.bfloat16)
    return high, low


def modes_of(share, groups):
    half = share // groups // 2
    order = []
    for group in range(groups):
        first = list(range(group * half, (group + 1) * half))
        order.append(first + [share - 1 - mode for mode in reversed(first)])
    return order


def split(values):
    high = values.astype(jnp.bfloat16)
    return high, (values - high.astype(jnp.float32)).astype(jnp.bfloat16)


def dot(a, b):
    return jnp.dot(a, b, preferred_element_type=jnp.float32)


def lines_along_z(lines, chunk, table):
    above, below = split(
        jnp.concatenate([lines[part, chunk] for part in range(lines.shape[0])], axis=1)
    )
    return dot(above, table[0]) + dot(above, table[1]) + dot(below, table[0])


def put(values, lines, table, factor, out, last, sem):
    share = values.shape[0]
    final = modes_of(share, GROUPS)[-1][-1]
    copies = [
        pltpu.make_async_copy(values.at[mode], out.at[mode], sem.at[mode])
        for mode in range(share)
        if mode != final
    ]
    for copy in copies:
        copy.start()
    last[...] = lines_along_z(lines, share - 1, table) * factor[...]
    copies.append(pltpu.make_async_copy(last, out.at[final], sem.at[final]))
    copies[-1].start()
    for copy in copies:
        copy.wait()


def kernel(
    rows,
    cols,
    field_hbm,
    table_x_hbm,
    table_y_hbm,
    table_z_hbm,
    symbol_x_hbm,
    symbol_y_hbm,
    symbol_z_hbm,
    out,
    lines_z,
    table_z,
    factor,
    field,
    high,
    low,
    table_x,
    table_y,
    symbol_x,
    symbol_y,
    symbol_z,
    symbol_yz,
    outgoing,
    lines_y,
    turned,
    field_sem,
    table_sem,
    row_send,
    row_recv,
    col_send,
    col_recv,
):
    row, col = lax.axis_index("row"), lax.axis_index("col")
    barrier = pltpu.get_barrier_semaphore()
    for step in range(1, rows):
        pl.semaphore_signal(
            barrier, inc=1, device_id=(lax.rem(row + step, rows), col), device_id_type=MESH
        )
    for step in range(1, cols):
        pl.semaphore_signal(
            barrier, inc=1, device_id=(row, lax.rem(col + step, cols)), device_id_type=MESH
        )
    share, part_y, _ = out.shape
    planes, _, half, wide = field.shape
    groups, _, _, lots, _ = outgoing.shape
    size = 2 * half
    in_group = share // groups
    middle = rows // 2
    upper = row // middle
    place = pl.multiple_of((row + upper * (rows + middle - 1 - 2 * row)) * planes, planes)

    side = math.isqrt(middle)
    chip, core = row // 2, lax.rem(row, 2)
    peers = []
    for target in CORES:
        for ahead, across in sorted(
            ((a, b) for a in range(side) for b in range(side)),
            key=lambda at: -sum(min(step, side - step) for step in at),
        )[:-1]:
            there = lax.rem(chip // side + ahead, side) * side + lax.rem(chip + across, side)
            peers.append(2 * there + target)
    peers.append(2 * chip + 1 - core)


    def load_of(plane, parity, source):
        return pltpu.make_async_copy(
            field_hbm.at[:, parity, source, :],
            field.at[plane, parity],
            field_sem.at[2 * plane + parity],
        )

    load_x = pltpu.make_async_copy(table_x_hbm, table_x, table_sem.at[0])
    load_x.start()

    def load_plane(plane, _):
        source = plane + upper * (planes - 1 - 2 * plane)
        for parity in range(2):
            load_of(plane, parity, source).start()
        return 0

    lax.fori_loop(0, planes, load_plane, 0)
    later = [
        pltpu.make_async_copy(source, target, table_sem.at[1 + at])
        for at, (source, target) in enumerate(
            [
                (table_y_hbm, table_y),
                (table_z_hbm, table_z),
                (symbol_x_hbm, symbol_x),
                (symbol_y_hbm, symbol_y),
                (symbol_z_hbm, symbol_z),
            ]
        )
    ]
    for load in later:
        load.start()
    def along_x(group, pair):
        parts = []
        for parity in range(2):
            mine = table_x.at[group, parity]
            both = dot(mine[...], high[pair, parity])
            parts.append(
                both[:lots] + both[lots:] + dot(mine[pl.ds(0, lots), :], low[pair, parity])
            )
        for sign, got in enumerate((parts[0] + parts[1], parts[0] - parts[1])):
            outgoing[group, sign, 2 * pair] = got[:, :wide]
            outgoing[group, sign, 2 * pair + 1] = got[:, wide:]

    def lot_of(chunk, peer):
        group, at = chunk // in_group, lax.rem(chunk, in_group)
        sign = peer // middle
        lot = (at + sign * (in_group - 1 - 2 * at)) * middle + peer + sign * (rows - 1 - 2 * peer)
        return group, sign, lot

    def send_row(chunk, first=0, count=planes):
        for peer in peers:
            group, sign, lot = lot_of(chunk, peer)
            pltpu.make_async_remote_copy(
                src_ref=outgoing.at[group, sign, pl.ds(first, count), lot, :],
                dst_ref=lines_y.at[chunk, pl.ds(place + first, count), :],
                send_sem=row_send,
                recv_sem=row_recv.at[chunk],
                device_id=(peer, col),
                device_id_type=MESH,
            ).start()

        group, sign, lot = lot_of(chunk, row)
        for plane in range(first, first + count):
            lines_y[chunk, pl.ds(place + plane, 1), :] = outgoing[
                group, sign, plane, pl.ds(lot, 1), :
            ]

    load_x.wait()
    for pair in range(planes // 2):
        for parity in range(2):
            load_of(2 * pair, parity, 2 * pair).wait()
            load_of(2 * pair + 1, parity, 2 * pair + 1).wait()
            both = jnp.concatenate([field[2 * pair, parity], field[2 * pair + 1, parity]], axis=1)
            high[pair, parity], low[pair, parity] = split(both)
        along_x(0, pair)
        if pair == planes // 4 - 1:
            pl.semaphore_wait(barrier, rows - 1 + cols - 1)
            send_row(0, 0, planes // 2)
    send_row(0, planes // 2, planes // 2)

    def send_first(chunk, _):
        send_row(chunk)
        return 0

    lax.fori_loop(1, in_group, send_first, 0)

    for load in later:
        load.wait()
    mine_y = jnp.broadcast_to(
        symbol_y[:, pl.ds(pl.multiple_of(col * part_y, part_y), part_y)], (part_y, part_y)
    )
    symbol_yz[...] = jnp.transpose(mine_y)[:, :1] + symbol_z[...]

    def along_y(chunk):
        arrived = lines_y.at[chunk, pl.ds(0, size - planes), :]
        pltpu.make_async_remote_copy(
            arrived, arrived, row_send, row_recv.at[chunk], device_id=(row, col), device_id_type=MESH
        ).wait_recv()
        first, second = lines_y[chunk, pl.ds(0, half), :], lines_y[chunk, pl.ds(half, half), :]
        above, below = split(jnp.concatenate([first + second, first - second], axis=1))
        got = dot(table_y[0], above) + dot(table_y[1], above) + dot(table_y[0], below)
        turned[chunk, pl.ds(0, half, 2), :] = got[:half, :wide]
        turned[chunk, pl.ds(1, half, 2), :] = got[half:, wide:]
        for step in range(cols - 1):
            peer = step + (col <= step).astype(jnp.int32)
            pltpu.make_async_remote_copy(
                src_ref=turned.at[
                    chunk, pl.ds(pl.multiple_of(peer * part_y, part_y), part_y), :
                ],
                dst_ref=lines_z.at[col, chunk],
                send_sem=col_send,
                recv_sem=col_recv.at[chunk],
                device_id=(row, peer),
                device_id_type=MESH,
            ).start()
        lines_z[col, chunk] = turned[
            chunk, pl.ds(pl.multiple_of(col * part_y, part_y), part_y), :
        ]

    def wait_col(chunk):
        arrived = lines_z.at[pl.ds(0, cols - 1), chunk]
        pltpu.make_async_remote_copy(
            arrived, arrived, col_send, col_recv.at[chunk], device_id=(row, col), device_id_type=MESH
        ).wait_recv()

    def factor_of(mode):
        return 2.0 / (1.0 + 0.2 * (symbol_x[row * share + mode] + symbol_yz[...])) - 1.0

    def along_z(chunk):
        wait_col(chunk)
        group, at = chunk // in_group, lax.rem(chunk, in_group)
        tail = at // (in_group // 2)
        mode = group * (in_group // 2) + at + tail * (share - in_group - group * in_group)
        out[mode] = lines_along_z(lines_z, chunk, table_z) * factor_of(mode)

    def step(chunk, _):
        along_y(chunk)

        for group in range(1, groups):

            @pl.when(chunk == (group - 1) * in_group + 1)
            def _():
                for pair in range(planes // 2):
                    along_x(group, pair)

        @pl.when(jnp.logical_and(chunk >= 1, chunk + in_group - 1 < share))
        def _():
            send_row(chunk + in_group - 1)

        @pl.when(chunk >= BEHIND)
        def _():
            along_z(chunk - BEHIND)

        return 0

    lax.fori_loop(0, share, step, 0)

    def last(chunk, _):
        along_z(chunk)
        return 0

    factor[...] = factor_of(modes_of(share, groups)[-1][-1])
    lax.fori_loop(share - BEHIND, share - 1, last, 0)
    wait_col(share - 1)
    all_rows = lines_y.at[:, pl.ds(0, size - planes), :]
    pltpu.make_async_remote_copy(
        all_rows, all_rows, row_send, row_recv.at[0], device_id=(row, col), device_id_type=MESH
    ).wait_send()
    all_cols = lines_z.at[pl.ds(0, cols - 1)]
    pltpu.make_async_remote_copy(
        all_cols, all_cols, col_send, col_recv.at[0], device_id=(row, col), device_id_type=MESH
    ).wait_send()


def per_device(rows, cols, field, symbol_x, symbol_y, symbol_z):
    size, planes, wide = field.shape
    share, part_y = size // rows, size // cols
    half, middle = size // 2, rows // 2

    table = transform_table(size)
    high, low = halves(table)
    order = np.asarray(modes_of(share, GROUPS))
    lots = order.shape[1] * middle
    wanted = (order[:, :, None] + share * np.arange(middle)).reshape(GROUPS, lots)
    table_x = np.stack(
        [np.concatenate([part[wanted] for part in (high, low)], axis=1)[:, :, parity::2] for parity in (0, 1)],
        axis=1,
    )
    table_y = np.stack(
        [np.concatenate([part[0::2, :half], part[1::2, :half]]) for part in (high, low)]
    )
    table_z = np.stack([high, low])

    anywhere = pl.BlockSpec(memory_space=pl.ANY)
    vmem = pl.BlockSpec(memory_space=pltpu.VMEM)
    made = pl.pallas_call(
        functools.partial(kernel, rows, cols),
        out_shape=(
            pltpu.VMEM((share, part_y, size), jnp.float32),
            pltpu.VMEM((cols, share, part_y, wide), jnp.float32),
            pltpu.VMEM(table_z.shape, jnp.bfloat16),
            pltpu.VMEM((part_y, size), jnp.float32),
        ),
        in_specs=[anywhere] * 7,
        out_specs=(vmem,) * 4,
        scratch_shapes=[
            pltpu.VMEM((planes, 2, half, wide), jnp.float32),
            pltpu.VMEM((planes // 2, 2, half, 2 * wide), jnp.bfloat16),
            pltpu.VMEM((planes // 2, 2, half, 2 * wide), jnp.bfloat16),
            pltpu.VMEM(table_x.shape, jnp.bfloat16),
            pltpu.VMEM(table_y.shape, jnp.bfloat16),
            pltpu.SMEM((size,), jnp.float32),
            pltpu.VMEM((1, size), jnp.float32),
            pltpu.VMEM((1, size), jnp.float32),
            pltpu.VMEM((part_y, size), jnp.float32),
            pltpu.VMEM((GROUPS, 2, planes, lots, wide), jnp.float32),
            pltpu.VMEM((share, size, wide), jnp.float32),
            pltpu.VMEM((share, size, wide), jnp.float32),
            pltpu.SemaphoreType.DMA((2 * planes,)),
            pltpu.SemaphoreType.DMA((6,)),
            pltpu.SemaphoreType.DMA,
            pltpu.SemaphoreType.DMA((share,)),
            pltpu.SemaphoreType.DMA,
            pltpu.SemaphoreType.DMA((share,)),
        ],
        compiler_params=pltpu.CompilerParams(
            collective_id=0, has_side_effects=True, vmem_limit_bytes=VMEM_LIMIT
        ),
        name="modes",
    )(
        *(
            pltpu.with_memory_space_constraint(operand, pltpu.HBM)
            for operand in (
                field.reshape(half, 2, planes, wide),
                jnp.asarray(table_x),
                jnp.asarray(table_y),
                jnp.asarray(table_z),
                symbol_x,
                symbol_y[None, :],
                symbol_z[None, :],
            )
        )
    )
    return pl.pallas_call(
        put,
        out_shape=pltpu.HBM((share, part_y, size), jnp.float32),
        in_specs=[vmem] * 4,
        out_specs=pl.BlockSpec(memory_space=pltpu.HBM),
        scratch_shapes=[
            pltpu.VMEM((part_y, size), jnp.float32),
            pltpu.SemaphoreType.DMA((share,)),
        ],
        compiler_params=pltpu.CompilerParams(vmem_limit_bytes=8 << 20),
        name="put",
    )(*(pltpu.with_memory_space_constraint(part, pltpu.VMEM) for part in made))


def solution(mesh):
    rows, cols = mesh.shape["row"], mesh.shape["col"]
    return jax.shard_map(
        functools.partial(per_device, rows, cols),
        mesh=mesh,
        in_specs=(P(None, "row", "col"), P(), P(), P()),
        out_specs=P("row", "col", None),
        check_vma=False,
    )
```
